32 devices in a mesh: zero: 8 (over z, x), width: 4 (over y, core).
Axes of the slice: x: 2, y: 2, z: 4, core: 2. Of those that a mesh axis runs over, the one named last changes fastest.
Arguments:
- weight_up: bfloat16 [12288, 49152], P('zero', 'width'), may hold values from -0.078125 to 0.078125
- low_up: bfloat16 [12288, 64], P('zero'), may hold values from -0.0546875 to 0.0546875
- high_up: bfloat16 [64, 49152], P(None, 'width'), may hold values from -0.75 to 0.75
- norm_train: float32 [12288], P(('zero', 'width')), may hold values from 0.25 to 1.75
- norm_step: float32 [12288], P(('zero', 'width')), may hold values from -0.3 to 0.3
Outputs:
- ready_up: bfloat16 [12288, 49152], P(None, ('width', 'zero'))
- scale_up: float32 [49152], P(('width', 'zero'))
- serve_norm: bfloat16 [12288], replicated
The draws below stay inside these ranges and needn't reach their ends.
All inputs are finite; a program needn't handle non-finite values. Where the reference program divides by a largest or mean magnitude, that divisor is 1e-20 or more.
Results may differ from the reference program's by a relative error of at most 0.001.
Values may be sent and summed in bfloat16 or wider, within the bound.
No kernel may reach another device: no remote copies, remote signals or barrier semaphores. Data moves between devices by JAX's collectives and lax.ppermute only.
A program may use at most 192 MiB of HBM per device.

```python
import jax
import jax.numpy as jnp

D_MODEL = 12288
D_INNER = 49152
RANK = 64


def with_spikes(array, key, source, target, blocks, factor):
    def block_of(axis_at):
        return (jnp.arange(array.shape[axis_at]) // (array.shape[axis_at] // blocks)).reshape((-1,) + (1,) * (array.ndim - 1 - axis_at))

    one_side = jax.random.permutation(key, blocks)[block_of(target)]
    far = (block_of(target) + blocks // 2) % blocks
    return jnp.where((block_of(source) == one_side) | (block_of(source) == far), factor * array, array)


def level_of(own_key, dims, shards, low, top_value):
    factor_of, own = 1.0, jax.random.fold_in(own_key, 6)
    for position, blocks in shards:
        draws = jnp.exp(jax.random.uniform(jax.random.fold_in(own, position), (blocks,), jnp.float32, low / len(shards), top_value / len(shards)))
        factor_of = factor_of * jnp.repeat(draws, dims[position] // blocks).reshape([-1 if axis == position else 1 for axis in range(len(dims))])
    return factor_of


def scatter_about(stream_key, shape, spread, most, shards=(), dtype=jnp.bfloat16):
    level = level_of(stream_key, shape, shards, -0.22, 0.18) if shards else 1.0
    entries = jax.random.normal(stream_key, shape, jnp.float32) * spread * level
    return jnp.minimum(jnp.maximum(entries, -most), most).astype(dtype)


def bell_draw_with(key, extent, width, reach, split, heavy, dtype=jnp.bfloat16):
    result = width * jax.random.normal(key, extent, jnp.float32)
    if split:
        result = result * level_of(key, extent, split, -0.22, 0.18)
    return jnp.clip(with_spikes(result, jax.random.fold_in(key, 3), *heavy), -reach, reach).astype(dtype)


def setup_inputs(seed: int = 0) -> dict:
    splits = jax.random.split(jax.random.key(seed), 6)
    return {
        "weight_up": bell_draw_with(splits[0], (D_MODEL, D_INNER), D_MODEL ** -0.5, 0.078125, ((0, 8), (1, 4)), (0, 1, 8, 2.0)),
        "low_up": scatter_about(splits[1], (D_MODEL, RANK), D_MODEL ** -0.5, 0.0546875, ((0, 8),)),
        "high_up": scatter_about(splits[2], (RANK, D_INNER), RANK ** -0.5, 0.75, ((1, 4),)),
        "norm_train": jnp.clip(1.0 + 0.15 * jax.random.normal(splits[3], (D_MODEL,), jnp.float32), 0.25, 1.75),
        "norm_step": jnp.clip(jax.random.uniform(splits[4], (D_MODEL,), jnp.float32, -0.3, 0.3) * level_of(splits[4], (D_MODEL,), ((0, 32),), -0.4, 0.0), -0.3, 0.3),
    }


mix_rate = 2.0


def reference(weight_up, low_up, high_up, norm_train, norm_step):
    latest_up = weight_up.astype(jnp.float32) + mix_rate * jnp.dot(low_up, high_up, preferred_element_type=jnp.float32)
    scale_up = jnp.max(jnp.abs(latest_up), axis=0)
    ready_up = (latest_up / scale_up).astype(jnp.bfloat16)
    serve_norm = (norm_train + norm_step).astype(jnp.bfloat16)
    return ready_up, scale_up, serve_norm
```

```python
import functools

import jax
import jax.numpy as jnp
from jax import lax
from jax.experimental import pallas as pl
from jax.experimental.pallas import tpu as pltpu
from jax.sharding import PartitionSpec as P

mix_rate = 2.0
LANES = 128
FINAL = (1, 4, None, 2, 1)
EARLY = (1, None)


def exchange(array, axis, size, step):
    return lax.ppermute(array, axis, [(i, i ^ step) for i in range(size)])


def slice_at(array, axis, start, size):
    starts, sizes = [0] * array.ndim, list(array.shape)
    starts[axis], sizes[axis] = start, size
    return lax.dynamic_slice(array, starts, sizes, allow_negative_indices=False)


def after(array, *others):
    return lax.optimization_barrier((array, *others))[0]


def tile_of(rows):
    return next(tile for tile in range(min(rows, 1536), 0, -1) if rows % tile == 0)


def merge_kernel(sources, rows, me_ref, *refs):
    n = len(sources)
    pieces, (low_ref, high_ref), refs = refs[:n], refs[n : n + 2], refs[n + 2 :]
    out_ref, scale_ref, latest = refs[-3:]
    me = me_ref[0]
    width = out_ref.shape[1]
    tile = tile_of(rows)
    top = jnp.zeros((8, width), jnp.float32)
    for piece, d in zip(pieces, sources):

        def product(t, top, piece=piece, d=d):
            at = pl.ds(pl.multiple_of(t * tile, tile), tile)
            here = pl.ds(pl.multiple_of(d * rows + t * tile, tile), tile)
            delta = jnp.dot(low_ref[here, :], high_ref[...], preferred_element_type=jnp.float32)
            value = piece[at, :].astype(jnp.float32) + mix_rate * delta
            latest[here, :] = value
            return jnp.maximum(top, jnp.max(jnp.abs(value).reshape(tile // 8, 8, width), axis=0))

        top = lax.fori_loop(0, rows // tile, product, top)
    scale = jnp.max(top, axis=0, keepdims=True)
    scale_ref[...] = scale
    inverse = 1.0 / scale
    for d in range(n):
        base = (me ^ d) * rows

        def ready(t, carry, d=d, base=base):
            here = pl.ds(pl.multiple_of(d * rows + t * tile, tile), tile)
            there = pl.ds(pl.multiple_of(base + t * tile, tile), tile)
            out_ref[there, :] = (latest[here, :] * inverse).astype(jnp.bfloat16)
            return carry

        lax.fori_loop(0, rows // tile, ready, 0)


def merge_chunk(me, pieces, low_all, high_part, offset, width, total, previous):
    sources = [d for d, _, _ in pieces]
    n, rows = len(pieces), pieces[0][2].shape[0]
    rank = low_all.shape[1]
    block = LANES if width % LANES == 0 else width
    steps, first = width // block, offset // block
    all_rows = n * rows
    in_specs = [
        pl.BlockSpec((rows, block), lambda j, me, at=(offset - start) // block: (0, at + j)) for _, start, _ in pieces
    ]
    in_specs.append(pl.BlockSpec((all_rows, rank), lambda j, me: (0, 0)))
    in_specs.append(pl.BlockSpec((rank, block), lambda j, me: (0, first + j)))
    operands = [*(array for _, _, array in pieces), low_all, high_part]
    aliases = {}
    if previous is not None:
        in_specs += [pl.BlockSpec(memory_space=pl.ANY)] * 2
        aliases = {1 + len(operands): 0, 2 + len(operands): 1}
        operands += previous
    return pl.pallas_call(
        functools.partial(merge_kernel, sources, rows),
        out_shape=(
            jax.ShapeDtypeStruct((all_rows, total), jnp.bfloat16),
            jax.ShapeDtypeStruct((1, total), jnp.float32),
        ),
        grid_spec=pltpu.PrefetchScalarGridSpec(
            num_scalar_prefetch=1,
            grid=(steps,),
            in_specs=in_specs,
            out_specs=(
                pl.BlockSpec((all_rows, block), lambda j, me: (0, first + j)),
                pl.BlockSpec((1, block), lambda j, me: (0, first + j)),
            ),
            scratch_shapes=[pltpu.VMEM((all_rows, block), jnp.float32)],
        ),
        input_output_aliases=aliases,
        compiler_params=pltpu.CompilerParams(
            dimension_semantics=("arbitrary",), vmem_limit_bytes=48 * 1024 * 1024
        ),
        cost_estimate=pl.CostEstimate(
            flops=2 * all_rows * rank * width, bytes_accessed=4 * all_rows * width, transcendentals=0
        ),
        name=f"merge_{offset}",
    )(me, *operands)


def cut(columns, parts):
    left = columns // LANES - sum(p or 0 for p in parts)
    if columns % LANES or left < 1:
        return [(0, columns)]
    widths = [LANES * (left if p is None else p) for p in parts]
    return [(sum(widths[:i]), width) for i, width in enumerate(widths)]


def shards(n, m, weight_up, low_up, high_up, norm_train, norm_step):
    me, mine = lax.axis_index("zero"), lax.axis_index("width")
    rows, rank = low_up.shape
    columns = weight_up.shape[1] // n
    part, half = rows // m, n // 2

    straight = [d for d in range(half, n) if d % 2 == 0]
    corner = [d for d in range(half, n) if d % 2 == 1]
    near = list(range(1, half))
    final = cut(columns, FINAL)
    early = cut(columns, EARLY)

    def send(weight, ds, spans):
        slices = [
            (d, start, slice_at(weight, 1, (me ^ d) * columns + start, width)) for start, width in spans for d in ds
        ]
        return slices, [(d, start, exchange(s, "zero", n, d) if d else s) for d, start, s in slices]

    weight, sent = weight_up, []
    for ds, spans in [(straight, [span]) for span in early] + [(near, [(0, columns)])] + [(corner, [span]) for span in final]:
        slices, received = send(weight, ds, spans)
        sent += received
        weight = after(weight, *(s for _, _, s in slices))
        if len(sent) == len(straight):
            low_up, norm_train = lax.optimization_barrier((low_up, norm_train, *(s for _, _, s in slices)))[:2]
    sent += send(weight, [0], [(0, columns)])[1]

    own = slice_at(low_up, 0, mine * part, part)
    gain = (norm_train + norm_step).astype(jnp.bfloat16)
    own = jnp.concatenate([own.T, gain[None, :]], axis=0)
    pair = jnp.stack([own, exchange(own, "zero", n, half)])
    pairs = jnp.stack([pair] + [exchange(pair, "zero", n, d) for d in range(1, half)], axis=1)
    along = pairs.reshape(n, rank + 1, part)
    spread = jnp.stack([along] + [exchange(along, "width", m, e) for e in range(1, m)])
    spread = jnp.concatenate([slice_at(spread, 0, mine ^ v, 1) for v in range(m)])
    low_all = spread[:, :, :rank, :].transpose(1, 0, 3, 2).reshape(n * rows, rank)
    gains = spread[:, :, rank, :]
    gains = jnp.concatenate([slice_at(gains, 1, me ^ s, 1) for s in range(n)], axis=1)
    serve_norm = gains.transpose(1, 0, 2).reshape(-1)

    high_part = slice_at(high_up, 1, me * columns, columns)
    result = None
    place = me.reshape(1).astype(jnp.int32)
    for offset, width in final:
        pieces = [(d, start, s) for d, start, s in sent if start <= offset and offset + width <= start + s.shape[1]]
        result = merge_chunk(place, pieces, low_all, high_part, offset, width, columns, result)
    ready_up, scale_up = result
    return ready_up, scale_up.reshape(-1), serve_norm


def solution(mesh):
    return jax.shard_map(
        functools.partial(shards, mesh.shape["zero"], mesh.shape["width"]),
        mesh=mesh,
        in_specs=(
            P("zero", "width"),
            P("zero", None),
            P(None, "width"),
            P(("zero", "width")),
            P(("zero", "width")),
        ),
        out_specs=(P(None, ("width", "zero")), P(("width", "zero")), P()),
        check_vma=False,
    )
```

```python
import functools

import jax
import jax.numpy as jnp
from jax import lax
from jax.experimental import pallas as pl
from jax.experimental.pallas import tpu as pltpu
from jax.sharding import PartitionSpec as P

mix_rate = 2.0
LANES = 128
FINAL = (1, 4, None, 2, 1)
EARLY = (1, None)


def exchange(array, axis, size, step):
    return lax.ppermute(array, axis, [(i, i ^ step) for i in range(size)])


def slice_at(array, axis, start, size):
    starts, sizes = [0] * array.ndim, list(array.shape)
    starts[axis], sizes[axis] = start, size
    return lax.dynamic_slice(array, starts, sizes, allow_negative_indices=False)


def after(array, *others):
    return lax.optimization_barrier((array, *others))[0]


def tile_of(rows):
    return next(tile for tile in range(min(rows, 1536), 0, -1) if rows % tile == 0)


def add_product(pieces, lows, high, latest, top):
    rows, width = pieces[0].shape
    tile = tile_of(rows)
    for i, (piece, low) in enumerate(zip(pieces, lows)):

        def product(t, top, i=i, piece=piece, low=low):
            at = pl.ds(pl.multiple_of(t * tile, tile), tile)
            delta = jnp.dot(low[at, :], high, preferred_element_type=jnp.float32)
            value = piece[at, :].astype(jnp.float32) + mix_rate * delta
            latest[pl.ds(pl.multiple_of(i * rows + t * tile, tile), tile), :] = value
            return jnp.maximum(top, jnp.max(jnp.abs(value).reshape(tile // 8, 8, width), axis=0))

        top = lax.fori_loop(0, rows // tile, product, top)
    return top


def merge_kernel(sources, rows, me_ref, *refs):
    n = len(sources)
    pieces, (low_ref, high_ref), refs = refs[:n], refs[n : n + 2], refs[n + 2 :]
    out_ref, scale_ref, latest = refs[-3:]
    me = me_ref[0]
    width = out_ref.shape[1]
    tile = tile_of(rows)
    lows = [low_ref.at[pl.ds(d * rows, rows), :] for d in sources]
    top = add_product(pieces, lows, high_ref[...], latest, jnp.zeros((8, width), jnp.float32))
    scale = jnp.max(top, axis=0, keepdims=True)
    scale_ref[...] = scale
    inverse = 1.0 / scale
    for i, d in enumerate(sources):
        base = (me ^ d) * rows

        def ready(t, carry, i=i, base=base):
            here = pl.ds(pl.multiple_of(i * rows + t * tile, tile), tile)
            there = pl.ds(pl.multiple_of(base + t * tile, tile), tile)
            out_ref[there, :] = (latest[here, :] * inverse).astype(jnp.bfloat16)
            return carry

        lax.fori_loop(0, rows // tile, ready, 0)


def begin_kernel(early, late, rows, *refs):
    n = len(early)
    pieces, (low_ref, high_ref), (latest, deltas, top) = refs[:n], refs[n : n + 2], refs[n + 2 :]
    lows = [low_ref.at[pl.ds(d * rows, rows), :] for d in early]
    top[...] = add_product(pieces, lows, high_ref[...], latest, jnp.zeros(top.shape, jnp.float32))
    for i, d in enumerate(late):
        low = low_ref[pl.ds(d * rows, rows), :]
        deltas[pl.ds(i * rows, rows), :] = mix_rate * jnp.dot(low, high_ref[...], preferred_element_type=jnp.float32)


def finish_kernel(early, late, rows, offset, me_ref, *refs):
    k = len(late)
    pieces, (begun, deltas, top_ref, scales, _, out_ref, scale_ref, latest, staged, sems) = refs[:k], refs[k:]
    me = me_ref[0]
    width = latest.shape[1]
    top = top_ref[...]
    for i, piece in enumerate(pieces):
        here = pl.ds(i * rows, rows)
        value = piece[...].astype(jnp.float32) + deltas[here, :]
        latest[here, :] = value
        top = jnp.maximum(top, jnp.max(jnp.abs(value).reshape(rows // 8, 8, width), axis=0))
    scale = jnp.max(top, axis=0, keepdims=True)
    inverse = 1.0 / scale
    copies = []
    for i, d in enumerate(early + late):
        source, at = (begun, i) if i < len(early) else (latest, i - len(early))
        here = pl.ds(i * rows, rows)
        staged[here, :] = (source[pl.ds(at * rows, rows), :] * inverse).astype(jnp.bfloat16)
        there = pl.ds(pl.multiple_of((me ^ d) * rows, rows), rows)
        copies.append(
            pltpu.make_async_copy(staged.at[here, :], out_ref.at[there, pl.ds(offset, width)], sems.at[i])
        )
        if i:
            copies[i - 1].start()
    copies[-1].start()
    for start in range(0, scales.shape[1], LANES):
        part = scale if start == offset else scales[:, pl.ds(start, LANES)]
        scale_ref[pl.ds(start, LANES)] = part[0]
    for copy in copies:
        copy.wait()


def merge_chunk(me, pieces, low_all, high_part, offset, width, total, previous):
    sources = [d for d, _, _ in pieces]
    n, rows = len(pieces), pieces[0][2].shape[0]
    rank = low_all.shape[1]
    block = LANES if width % LANES == 0 else width
    steps, first = width // block, offset // block
    all_rows = n * rows
    in_specs = [
        pl.BlockSpec((rows, block), lambda j, me, at=(offset - start) // block: (0, at + j)) for _, start, _ in pieces
    ]
    in_specs.append(pl.BlockSpec((all_rows, rank), lambda j, me: (0, 0)))
    in_specs.append(pl.BlockSpec((rank, block), lambda j, me: (0, first + j)))
    operands = [*(array for _, _, array in pieces), low_all, high_part]
    aliases = {}
    if previous is not None:
        in_specs += [pl.BlockSpec(memory_space=pl.ANY)] * 2
        aliases = {1 + len(operands): 0, 2 + len(operands): 1}
        operands += previous
    return pl.pallas_call(
        functools.partial(merge_kernel, sources, rows),
        out_shape=(
            jax.ShapeDtypeStruct((all_rows, total), jnp.bfloat16),
            jax.ShapeDtypeStruct((1, total), jnp.float32),
        ),
        grid_spec=pltpu.PrefetchScalarGridSpec(
            num_scalar_prefetch=1,
            grid=(steps,),
            in_specs=in_specs,
            out_specs=(
                pl.BlockSpec((all_rows, block), lambda j, me: (0, first + j)),
                pl.BlockSpec((1, block), lambda j, me: (0, first + j)),
            ),
            scratch_shapes=[pltpu.VMEM((all_rows, block), jnp.float32)],
        ),
        input_output_aliases=aliases,
        compiler_params=pltpu.CompilerParams(
            dimension_semantics=("arbitrary",), vmem_limit_bytes=32 * 1024 * 1024
        ),
        cost_estimate=pl.CostEstimate(
            flops=2 * all_rows * rank * width, bytes_accessed=4 * all_rows * width, transcendentals=0
        ),
        name=f"merge_{offset}",
    )(me, *operands)


def merge_last(me, early, late, low_all, high_part, offset, width, total, previous):
    rows, rank = late[0][2].shape[0], low_all.shape[1]
    begun_rows, all_rows = len(early) * rows, low_all.shape[0]
    at_of = lambda start: (offset - start) // width
    whole = pl.BlockSpec(memory_space=pltpu.VMEM)
    params = pltpu.CompilerParams(dimension_semantics=("arbitrary",), vmem_limit_bytes=28 * 1024 * 1024)

    def cost(merged, written):
        return pl.CostEstimate(
            flops=2 * merged * rank * width, bytes_accessed=2 * (merged + written) * width, transcendentals=0
        )

    begun, deltas, top = pl.pallas_call(
        functools.partial(begin_kernel, [d for d, _, _ in early], [d for d, _, _ in late], rows),
        out_shape=(
            jax.ShapeDtypeStruct((begun_rows, width), jnp.float32),
            jax.ShapeDtypeStruct((all_rows - begun_rows, width), jnp.float32),
            jax.ShapeDtypeStruct((8, width), jnp.float32),
        ),
        grid=(1,),
        in_specs=[
            *(pl.BlockSpec((rows, width), lambda j, at=at_of(start): (0, at)) for _, start, _ in early),
            pl.BlockSpec((all_rows, rank), lambda j: (0, 0)),
            pl.BlockSpec((rank, width), lambda j: (0, offset // width)),
        ],
        out_specs=(whole, whole, whole),
        compiler_params=params,
        cost_estimate=cost(all_rows, 2 * all_rows),
        name="merge_begin",
    )(*(array for _, _, array in early), low_all, high_part)

    k = len(late)
    return pl.pallas_call(
        functools.partial(finish_kernel, [d for d, _, _ in early], [d for d, _, _ in late], rows, offset),
        out_shape=(
            jax.ShapeDtypeStruct((all_rows, total), jnp.bfloat16),
            jax.ShapeDtypeStruct((total,), jnp.float32),
        ),
        grid_spec=pltpu.PrefetchScalarGridSpec(
            num_scalar_prefetch=1,
            grid=(1,),
            in_specs=[
                *(pl.BlockSpec((rows, width), lambda j, me, at=at_of(start): (0, at)) for _, start, _ in late),
                whole,
                whole,
                whole,
                whole,
                pl.BlockSpec(memory_space=pl.ANY),
            ],
            out_specs=(pl.BlockSpec(memory_space=pl.ANY), whole),
            scratch_shapes=[
                pltpu.VMEM((k * rows, width), jnp.float32),
                pltpu.VMEM((all_rows, width), jnp.bfloat16),
                pltpu.SemaphoreType.DMA((len(early) + k,)),
            ],
        ),
        input_output_aliases={k + 5: 0},
        compiler_params=params,
        cost_estimate=cost(k * rows, all_rows),
        name="merge_finish",
    )(me, *(array for _, _, array in late), begun, deltas, top, previous[1], previous[0])


def cut(columns, parts):
    left = columns // LANES - sum(p or 0 for p in parts)
    if columns % LANES or left < 1:
        return [(0, columns)]
    widths = [LANES * (left if p is None else p) for p in parts]
    return [(sum(widths[:i]), width) for i, width in enumerate(widths)]


def shards(n, m, weight_up, low_up, high_up, norm_train, norm_step):
    me, mine = lax.axis_index("zero"), lax.axis_index("width")
    rows, rank = low_up.shape
    columns = weight_up.shape[1] // n
    part, half = rows // m, n // 2

    straight = [d for d in range(half, n) if d % 2 == 0]
    corner = [d for d in range(half, n) if d % 2 == 1]
    near = list(range(1, half))
    final = cut(columns, FINAL)
    early = cut(columns, EARLY)

    def send(weight, ds, spans):
        slices = [
            (d, start, slice_at(weight, 1, (me ^ d) * columns + start, width)) for start, width in spans for d in ds
        ]
        return slices, [(d, start, exchange(s, "zero", n, d) if d else s) for d, start, s in slices]

    weight, sent = weight_up, []
    for ds, spans in [([d], [span]) for span in early for d in straight] + [(near, [(0, columns)])] + [(corner, [span]) for span in final]:
        slices, received = send(weight, ds, spans)
        sent += received
        weight = after(weight, *(s for _, _, s in slices))
        if len(sent) == len(straight):
            low_up, norm_train = lax.optimization_barrier((low_up, norm_train, *(s for _, _, s in slices)))[:2]
    sent += send(weight, [0], [(0, columns)])[1]

    own = slice_at(low_up, 0, mine * part, part)
    gain = (norm_train + norm_step).astype(jnp.bfloat16)
    own = jnp.concatenate([own.T, gain[None, :]], axis=0)
    pair = jnp.stack([own, exchange(own, "zero", n, half)])
    pairs = jnp.stack([pair] + [exchange(pair, "zero", n, d) for d in range(1, half)], axis=1)
    along = pairs.reshape(n, rank + 1, part)
    spread = jnp.stack([along] + [exchange(along, "width", m, e) for e in range(1, m)])
    spread = jnp.concatenate([slice_at(spread, 0, mine ^ v, 1) for v in range(m)])
    low_all = spread[:, :, :rank, :].transpose(1, 0, 3, 2).reshape(n * rows, rank)
    gains = spread[:, :, rank, :]
    gains = jnp.concatenate([slice_at(gains, 1, me ^ s, 1) for s in range(n)], axis=1)
    serve_norm = gains.transpose(1, 0, 2).reshape(-1)

    high_part = slice_at(high_up, 1, me * columns, columns)
    result = None
    place = me.reshape(1).astype(jnp.int32)
    for offset, width in final:
        pieces = [(d, start, s) for d, start, s in sent if start <= offset and offset + width <= start + s.shape[1]]
        if result is not None and offset + width == columns and width == LANES:
            early, late = [p for p in pieces if p[0] not in corner], [p for p in pieces if p[0] in corner]
            result = merge_last(place, early, late, low_all, high_part, offset, width, columns, result)
        else:
            result = merge_chunk(place, pieces, low_all, high_part, offset, width, columns, result)
    ready_up, scale_up = result
    return ready_up, scale_up.reshape(-1), serve_norm


def solution(mesh):
    return jax.shard_map(
        functools.partial(shards, mesh.shape["zero"], mesh.shape["width"]),
        mesh=mesh,
        in_specs=(
            P("zero", "width"),
            P("zero", None),
            P(None, "width"),
            P(("zero", "width")),
            P(("zero", "width")),
        ),
        out_specs=(P(None, ("width", "zero")), P(("width", "zero")), P()),
        check_vma=False,
    )
```

```python
import functools

import jax
import jax.numpy as jnp
from jax import lax
from jax.experimental import pallas as pl
from jax.experimental.pallas import tpu as pltpu
from jax.sharding import PartitionSpec as P

mix_rate = 2.0
LANES = 128
FINAL = (1, 4, None, 2, 1)


def exchange(array, axis, size, step):
    return lax.ppermute(array, axis, [(i, i ^ step) for i in range(size)])


def slice_at(array, axis, start, size):
    starts, sizes = [0] * array.ndim, list(array.shape)
    starts[axis], sizes[axis] = start, size
    return lax.dynamic_slice(array, starts, sizes, allow_negative_indices=False)


def after(array, *others):
    return lax.optimization_barrier((array, *others))[0]


def tile_of(rows):
    return next(tile for tile in range(min(rows, 1536), 0, -1) if rows % tile == 0)


def add_product(pieces, places, lows, high, latest, top):
    width = latest.shape[1]
    for piece, place, low in zip(pieces, places, lows):
        tile = tile_of(piece.shape[0])

        def product(t, top, piece=piece, place=place, low=low):
            at = pl.ds(pl.multiple_of(t * tile, 16), tile)
            delta = jnp.dot(low[at, :], high, preferred_element_type=jnp.float32)
            value = piece[at, :].astype(jnp.float32) + mix_rate * delta
            latest[pl.ds(pl.multiple_of(place + t * tile, 16), tile), :] = value
            return jnp.maximum(top, jnp.max(jnp.abs(value).reshape(tile // 8, 8, width), axis=0))

        top = lax.fori_loop(0, piece.shape[0] // tile, product, top)
    return top


def places_of(pieces, rows):
    sources = list(dict.fromkeys(d for d, _, _, _ in pieces))
    return sources, [sources.index(d) * rows + row for d, row, _, _ in pieces]


def lows_of(pieces, low_ref, rows):
    return [low_ref.at[pl.ds(d * rows + row, count), :] for d, row, count in pieces]


def merge_kernel(sources, places, spans, rows, me_ref, *refs):
    k = len(places)
    pieces, (low_ref, high_ref), refs = refs[:k], refs[k : k + 2], refs[k + 2 :]
    out_ref, scale_ref, latest = refs[-3:]
    me = me_ref[0]
    width = out_ref.shape[1]
    tile = tile_of(rows)
    lows = lows_of(spans, low_ref, rows)
    top = add_product(pieces, places, lows, high_ref[...], latest, jnp.zeros((8, width), jnp.float32))
    scale = jnp.max(top, axis=0, keepdims=True)
    scale_ref[...] = scale
    inverse = 1.0 / scale
    for i, d in enumerate(sources):
        base = (me ^ d) * rows

        def ready(t, carry, i=i, base=base):
            here = pl.ds(pl.multiple_of(i * rows + t * tile, 16), tile)
            there = pl.ds(pl.multiple_of(base + t * tile, 16), tile)
            out_ref[there, :] = (latest[here, :] * inverse).astype(jnp.bfloat16)
            return carry

        lax.fori_loop(0, rows // tile, ready, 0)


def write_out(values, me, sources, rows, offset, staged, out_ref, sems):
    copies = []
    for i, d in enumerate(sources):
        here, there = pl.ds(i * rows, rows), pl.ds(pl.multiple_of((me ^ d) * rows, 16), rows)
        staged[here, :] = values(i).astype(jnp.bfloat16)
        target = out_ref.at[there, pl.ds(offset, staged.shape[1])]
        copies.append(pltpu.make_async_copy(staged.at[here, :], target, sems.at[i]))
        if i:
            copies[i - 1].start()
    copies[-1].start()
    for copy in copies:
        copy.wait()


def begin_kernel(sources, places, spans, late, rows, offset, me_ref, *refs):
    k, peaks = len(places), len(late)
    pieces, refs = refs[:k], refs[k:]
    tops, (low_ref, high_ref, out_ref, scale_ref, inverse_ref, deltas, latest, staged, sems) = refs[:peaks], refs[peaks:]
    width = latest.shape[1]
    lows = lows_of(spans, low_ref, rows)
    top = add_product(pieces, places, lows, high_ref[...], latest, jnp.zeros((8, width), jnp.float32))
    scale = jnp.max(top, axis=0, keepdims=True)
    for late_top in tops:
        scale = jnp.maximum(scale, late_top[...])
    scale_ref[...] = scale
    inverse = 1.0 / scale
    inverse_ref[...] = inverse
    for i, d in enumerate(late):
        low = low_ref[pl.ds(d * rows, rows), :]
        deltas[pl.ds(i * rows, rows), :] = mix_rate * jnp.dot(low, high_ref[...], preferred_element_type=jnp.float32)
    values = lambda i: latest[pl.ds(i * rows, rows), :] * inverse
    write_out(values, me_ref[0], sources, rows, offset, staged, out_ref, sems)


def finish_kernel(late, places, rows, offset, me_ref, *refs):
    k = len(late)
    pieces, (deltas, inverse_ref, scales, _, out_ref, scale_ref, landed, staged, arrive, leave) = refs[:k], refs[k:]
    me, width = me_ref[0], staged.shape[1]
    size = rows // (arrive.shape[0] // k)
    parts = [(i, d, row) for i, d in enumerate(late) for row in range(0, rows, size)]
    ins, outs = [], []
    for j, (i, d, row) in enumerate(parts):
        source = pieces[i].at[pl.ds(row, size), pl.ds(places[i], width)]
        ins.append(pltpu.make_async_copy(source, landed.at[pl.ds(j * size, size), :], arrive.at[j]))
        ins[j].start()
    for start in range(0, scales.shape[1], LANES):
        scale_ref[pl.ds(start, LANES)] = scales[:, pl.ds(start, LANES)][0]
    inverse = inverse_ref[...]
    for j, (i, d, row) in enumerate(parts):
        here, there = pl.ds(j * size, size), pl.ds(pl.multiple_of((me ^ d) * rows + row, 16), size)
        ins[j].wait()
        staged[here, :] = ((landed[here, :].astype(jnp.float32) + deltas[here, :]) * inverse).astype(jnp.bfloat16)
        outs.append(pltpu.make_async_copy(staged.at[here, :], out_ref.at[there, pl.ds(offset, width)], leave.at[j]))
        if j:
            outs[j - 1].start()
    outs[-1].start()
    for copy in outs:
        copy.wait()


def cost_of(merged, written, rank, width):
    return pl.CostEstimate(
        flops=2 * merged * rank * width, bytes_accessed=2 * (merged + written) * width, transcendentals=0
    )


def params_of(mebibytes):
    return pltpu.CompilerParams(dimension_semantics=("arbitrary",), vmem_limit_bytes=mebibytes * 1024 * 1024)


def piece_specs(pieces, offset, block):
    return [
        pl.BlockSpec((array.shape[0], block), lambda j, me, at=(offset - start) // block: (0, at + j))
        for _, _, start, array in pieces
    ]


def spans_of(pieces):
    return [(d, row, array.shape[0]) for d, row, _, array in pieces]


def merge_chunk(me, pieces, rows, low_all, high_part, offset, width, previous):
    sources, places = places_of(pieces, rows)
    (all_rows, rank), total = low_all.shape, high_part.shape[1]
    block = LANES if width % LANES == 0 else width
    steps, first = width // block, offset // block
    in_specs = piece_specs(pieces, offset, block)
    in_specs.append(pl.BlockSpec((all_rows, rank), lambda j, me: (0, 0)))
    in_specs.append(pl.BlockSpec((rank, block), lambda j, me: (0, first + j)))
    operands = [*(array for _, _, _, array in pieces), low_all, high_part]
    aliases = {}
    if previous is not None:
        in_specs += [pl.BlockSpec(memory_space=pl.ANY)] * 2
        aliases = {1 + len(operands): 0, 2 + len(operands): 1}
        operands += previous
    return pl.pallas_call(
        functools.partial(merge_kernel, sources, places, spans_of(pieces), rows),
        out_shape=(
            jax.ShapeDtypeStruct((all_rows, total), jnp.bfloat16),
            jax.ShapeDtypeStruct((1, total), jnp.float32),
        ),
        grid_spec=pltpu.PrefetchScalarGridSpec(
            num_scalar_prefetch=1,
            grid=(steps,),
            in_specs=in_specs,
            out_specs=(
                pl.BlockSpec((all_rows, block), lambda j, me: (0, first + j)),
                pl.BlockSpec((1, block), lambda j, me: (0, first + j)),
            ),
            scratch_shapes=[pltpu.VMEM((all_rows, block), jnp.float32)],
        ),
        input_output_aliases=aliases,
        compiler_params=params_of(32),
        cost_estimate=cost_of(all_rows, all_rows, rank, width),
        name=f"merge_{offset}",
    )(me, *operands)


WHOLE = pl.BlockSpec(memory_space=pltpu.VMEM)


def merge_begin(me, pieces, late, peaks, rows, low_all, high_part, offset, width):
    sources, places = places_of(pieces, rows)
    (all_rows, rank), total = low_all.shape, high_part.shape[1]
    early_rows, late_rows = len(sources) * rows, len(late) * rows
    return pl.pallas_call(
        functools.partial(begin_kernel, sources, places, spans_of(pieces), late, rows, offset),
        out_shape=(
            jax.ShapeDtypeStruct((all_rows, total), jnp.bfloat16),
            jax.ShapeDtypeStruct((1, total), jnp.float32),
            jax.ShapeDtypeStruct((1, width), jnp.float32),
            jax.ShapeDtypeStruct((late_rows, width), jnp.float32),
        ),
        grid_spec=pltpu.PrefetchScalarGridSpec(
            num_scalar_prefetch=1,
            grid=(1,),
            in_specs=[
                *piece_specs(pieces, offset, width),
                *[WHOLE] * len(late),
                pl.BlockSpec((all_rows, rank), lambda j, me: (0, 0)),
                pl.BlockSpec((rank, width), lambda j, me: (0, offset // width)),
            ],
            out_specs=(
                pl.BlockSpec(memory_space=pl.ANY),
                pl.BlockSpec((1, width), lambda j, me: (0, offset // width)),
                WHOLE,
                WHOLE,
            ),
            scratch_shapes=[
                pltpu.VMEM((early_rows, width), jnp.float32),
                pltpu.VMEM((early_rows, width), jnp.bfloat16),
                pltpu.SemaphoreType.DMA((len(sources),)),
            ],
        ),
        compiler_params=params_of(32),
        cost_estimate=cost_of(all_rows, all_rows, rank, width),
        name="merge_begin",
    )(me, *(array for _, _, _, array in pieces), *peaks, low_all, high_part)


def merge_finish(me, pieces, rows, deltas, inverse, offset, width, previous):
    late, (all_rows, total) = [d for d, _, _, _ in pieces], previous[0].shape
    places = [offset - start for _, _, start, _ in pieces]
    parts = len(late) * (4 if rows % 64 == 0 else 1)
    return pl.pallas_call(
        functools.partial(finish_kernel, late, places, rows, offset),
        out_shape=(
            jax.ShapeDtypeStruct((all_rows, total), jnp.bfloat16),
            jax.ShapeDtypeStruct((total,), jnp.float32),
        ),
        grid_spec=pltpu.PrefetchScalarGridSpec(
            num_scalar_prefetch=1,
            grid=(1,),
            in_specs=[
                *[pl.BlockSpec(memory_space=pl.ANY)] * len(late),
                *[WHOLE] * 3,
                pl.BlockSpec(memory_space=pl.ANY),
            ],
            out_specs=(pl.BlockSpec(memory_space=pl.ANY), WHOLE),
            scratch_shapes=[
                pltpu.VMEM((len(late) * rows, width), jnp.bfloat16),
                pltpu.VMEM((len(late) * rows, width), jnp.bfloat16),
                pltpu.SemaphoreType.DMA((parts,)),
                pltpu.SemaphoreType.DMA((parts,)),
            ],
        ),
        input_output_aliases={len(late) + 4: 0},
        compiler_params=params_of(16),
        cost_estimate=cost_of(len(late) * rows, len(late) * rows, 1, width),
        name="merge_finish",
    )(me, *(array for _, _, _, array in pieces), deltas, inverse, previous[1], previous[0])


def lead_kernel(d, me_ref, weight_ref, out_ref, sems):
    rows, columns = out_ref.shape
    start = pl.multiple_of((me_ref[0] ^ d) * columns, LANES)
    copies = []
    for i in range(rows // 16):
        here = pl.ds(i * 16, 16)
        source = weight_ref.at[here, pl.ds(start, columns)]
        copies.append(pltpu.make_async_copy(source, out_ref.at[here, :], sems.at[i]))
        copies[i].start()
    for copy in copies:
        copy.wait()


def take_lead(me, weight, d, rows, columns):
    return pl.pallas_call(
        functools.partial(lead_kernel, d),
        out_shape=jax.ShapeDtypeStruct((rows, columns), weight.dtype),
        in_specs=[pl.BlockSpec(memory_space=pltpu.SMEM), pl.BlockSpec(memory_space=pltpu.MemorySpace.HBM)],
        out_specs=WHOLE,
        scratch_shapes=[pltpu.SemaphoreType.DMA((rows // 16,))],
        compiler_params=pltpu.CompilerParams(vmem_limit_bytes=48 * 1024 * 1024),
        name="lead",
    )(me.reshape(1).astype(jnp.int32), weight)


def cut(columns, parts):
    left = columns // LANES - sum(p or 0 for p in parts)
    if columns % LANES or left < 1:
        return [(0, columns)]
    widths = [LANES * (left if p is None else p) for p in parts]
    return [(sum(widths[:i]), width) for i, width in enumerate(widths)]


def shards(n, m, weight_up, low_up, high_up, norm_train, norm_step):
    me, mine = lax.axis_index("zero"), lax.axis_index("width")
    rows, rank = low_up.shape
    columns = weight_up.shape[1] // n
    part, half = rows // m, n // 2

    straight = [d for d in range(half, n) if d % 2 == 0]
    corner = [d for d in range(half, n) if d % 2 == 1]
    near = list(range(1, half))
    final = cut(columns, FINAL)
    offset, width = final[-1]
    ahead = len(final) > 1 and width == LANES
    lead = max(16, rows // 128 * 16)

    def take(weight, d, row, count, start, width):
        here = (row, (me ^ d) * columns + start)
        return d, row, start, lax.dynamic_slice(weight, here, (count, width), allow_negative_indices=False)

    groups = [[(d, 0, rows, 0, columns)] for d in straight]
    if groups:
        groups = [[(straight[0], 0, lead, 0, columns)], [(straight[0], lead, rows - lead, 0, columns)]] + groups[1:]
    groups += [[(d, 0, rows, 0, columns)] for d in near]
    weight, sent, low_own, gain_own, peaks = weight_up, [], low_up, norm_train, []
    for group in groups + [[(d, 0, rows, *span)] for span in final for d in corner]:
        if ahead and not peaks and group[0][0] in corner:
            tops, low_late = [], after(low_up, *arrays)
            for d in corner:
                late = take(weight_up, d, 0, rows, offset, width)[3].astype(jnp.float32)
                high = slice_at(high_up, 1, (me ^ d) * columns + offset, width)
                late += mix_rate * jnp.dot(low_late, high, preferred_element_type=jnp.float32)
                tops.append(jnp.max(jnp.abs(late), axis=0, keepdims=True))
            peaks = [exchange(top, "zero", n, d) for d, top in zip(corner, tops)]
            weight = after(weight, *tops)
        if weight is weight_up and columns % LANES == 0:
            last = [(d, row, start, take_lead(me, weight, d, count, width)) for d, row, count, start, width in group]
        else:
            last = [take(weight, *piece) for piece in group]
        arrays = [array for _, _, _, array in last]
        sent += [(d, row, start, exchange(array, "zero", n, d)) for d, row, start, array in last]
        if weight is weight_up:
            low_own, gain_own = lax.optimization_barrier((low_own, gain_own, *arrays))[:2]
        weight = after(weight, *arrays)
    sent.append(take(weight, 0, 0, rows, 0, columns))

    own = slice_at(low_own, 0, mine * part, part)
    gain = (gain_own + norm_step).astype(jnp.bfloat16)
    own = jnp.concatenate([own.T, gain[None, :]], axis=0)
    pair = jnp.stack([own, exchange(own, "zero", n, half)])
    pairs = jnp.stack([pair] + [exchange(pair, "zero", n, d) for d in range(1, half)], axis=1)
    along = pairs.reshape(n, rank + 1, part)
    spread = jnp.stack([along] + [exchange(along, "width", m, e) for e in range(1, m)])
    spread = jnp.concatenate([slice_at(spread, 0, mine ^ v, 1) for v in range(m)])
    low_all = spread[:, :, :rank, :].transpose(1, 0, 3, 2).reshape(n * rows, rank)
    gains = spread[:, :, rank, :]
    gains = jnp.concatenate([slice_at(gains, 1, me ^ s, 1) for s in range(n)], axis=1)
    serve_norm = gains.transpose(1, 0, 2).reshape(-1)

    high_part = slice_at(high_up, 1, me * columns, columns)
    place = me.reshape(1).astype(jnp.int32)

    def arrived(offset, width, ds):
        fits = lambda start, array: start <= offset and offset + width <= start + array.shape[1]
        return [piece for piece in sent if piece[0] in ds and fits(*piece[2:])]

    result = None
    if ahead:
        early = [d for d in range(n) if d not in corner]
        *result, inverse, deltas = merge_begin(
            place, arrived(offset, width, early), corner, peaks, rows, low_all, high_part, offset, width
        )
    for start, count in final[:-1] if ahead else final:
        pieces = arrived(start, count, range(n))
        result = merge_chunk(place, pieces, rows, low_all, high_part, start, count, result)
    if ahead:
        late = arrived(offset, width, corner)
        ready_up, scale_up = merge_finish(place, late, rows, deltas, inverse, offset, width, result)
    else:
        ready_up, scale_up = result
    return ready_up, scale_up.reshape(-1), serve_norm


def solution(mesh):
    return jax.shard_map(
        functools.partial(shards, mesh.shape["zero"], mesh.shape["width"]),
        mesh=mesh,
        in_specs=(
            P("zero", "width"),
            P("zero", None),
            P(None, "width"),
            P(("zero", "width")),
            P(("zero", "width")),
        ),
        out_specs=(P(None, ("width", "zero")), P(("width", "zero")), P()),
        check_vma=False,
    )
```

```python
import functools

import jax
import jax.numpy as jnp
from jax import lax
from jax.experimental import pallas as pl
from jax.experimental.pallas import tpu as pltpu
from jax.sharding import PartitionSpec as P

mix_rate = 2.0
LANES = 128
FINAL = (1, 4, None, 2, 1)


def exchange(array, axis, size, step):
    return lax.ppermute(array, axis, [(i, i ^ step) for i in range(size)])


def slice_at(array, axis, start, size):
    starts, sizes = [0] * array.ndim, list(array.shape)
    starts[axis], sizes[axis] = start, size
    return lax.dynamic_slice(array, starts, sizes, allow_negative_indices=False)


def after(array, *others):
    return lax.optimization_barrier((array, *others))[0]


def tile_of(rows):
    return next(tile for tile in range(min(rows, 1536), 0, -1) if rows % tile == 0)


def add_product(pieces, places, lows, high, latest, top):
    width = latest.shape[1]
    for piece, place, low in zip(pieces, places, lows):
        tile = tile_of(piece.shape[0])

        def product(t, top, piece=piece, place=place, low=low):
            at = pl.ds(pl.multiple_of(t * tile, 16), tile)
            delta = jnp.dot(low[at, :], high, preferred_element_type=jnp.float32)
            value = piece[at, :].astype(jnp.float32) + mix_rate * delta
            latest[pl.ds(pl.multiple_of(place + t * tile, 16), tile), :] = value
            return jnp.maximum(top, jnp.max(jnp.abs(value).reshape(tile // 8, 8, width), axis=0))

        top = lax.fori_loop(0, piece.shape[0] // tile, product, top)
    return top


def places_of(pieces, rows):
    sources = list(dict.fromkeys(d for d, _, _, _ in pieces))
    return sources, [sources.index(d) * rows + row for d, row, _, _ in pieces]


def lows_of(pieces, low_ref, rows):
    return [low_ref.at[pl.ds(d * rows + row, count), :] for d, row, count in pieces]


def merge_kernel(sources, places, spans, rows, me_ref, *refs):
    k = len(places)
    pieces, (low_ref, high_ref), refs = refs[:k], refs[k : k + 2], refs[k + 2 :]
    out_ref, scale_ref, latest = refs[-3:]
    me = me_ref[0]
    width = out_ref.shape[1]
    tile = tile_of(rows)
    lows = lows_of(spans, low_ref, rows)
    top = add_product(pieces, places, lows, high_ref[...], latest, jnp.zeros((8, width), jnp.float32))
    scale = jnp.max(top, axis=0, keepdims=True)
    scale_ref[...] = scale
    inverse = 1.0 / scale
    for i, d in enumerate(sources):
        base = (me ^ d) * rows

        def ready(t, carry, i=i, base=base):
            here = pl.ds(pl.multiple_of(i * rows + t * tile, 16), tile)
            there = pl.ds(pl.multiple_of(base + t * tile, 16), tile)
            out_ref[there, :] = (latest[here, :] * inverse).astype(jnp.bfloat16)
            return carry

        lax.fori_loop(0, rows // tile, ready, 0)


def write_out(values, me, sources, rows, offset, staged, out_ref, sems):
    copies = []
    for i, d in enumerate(sources):
        here, there = pl.ds(i * rows, rows), pl.ds(pl.multiple_of((me ^ d) * rows, 16), rows)
        staged[here, :] = values(i).astype(jnp.bfloat16)
        target = out_ref.at[there, pl.ds(offset, staged.shape[1])]
        copies.append(pltpu.make_async_copy(staged.at[here, :], target, sems.at[i]))
        if i:
            copies[i - 1].start()
    copies[-1].start()
    for copy in copies:
        copy.wait()


def begin_kernel(sources, places, spans, late, rows, offset, me_ref, *refs):
    k, peaks = len(places), len(late)
    pieces, refs = refs[:k], refs[k:]
    tops, (low_ref, high_ref, out_ref, scale_ref, inverse_ref, deltas, latest, staged, sems) = refs[:peaks], refs[peaks:]
    width = latest.shape[1]
    lows = lows_of(spans, low_ref, rows)
    top = add_product(pieces, places, lows, high_ref[...], latest, jnp.zeros((8, width), jnp.float32))
    scale = jnp.max(top, axis=0, keepdims=True)
    for late_top in tops:
        scale = jnp.maximum(scale, late_top[...])
    scale_ref[...] = scale
    inverse = 1.0 / scale
    inverse_ref[...] = inverse
    for i, d in enumerate(late):
        low = low_ref[pl.ds(d * rows, rows), :]
        deltas[pl.ds(i * rows, rows), :] = mix_rate * jnp.dot(low, high_ref[...], preferred_element_type=jnp.float32)
    values = lambda i: latest[pl.ds(i * rows, rows), :] * inverse
    write_out(values, me_ref[0], sources, rows, offset, staged, out_ref, sems)


def finish_kernel(late, places, rows, offset, me_ref, *refs):
    k = len(late)
    pieces, (deltas, inverse_ref, scales, _, out_ref, scale_ref, landed, staged, arrive, leave) = refs[:k], refs[k:]
    me, width = me_ref[0], staged.shape[1]
    size = rows // (arrive.shape[0] // k)
    parts = [(i, d, row) for i, d in enumerate(late) for row in range(0, rows, size)]
    ins, outs = [], []
    for j, (i, d, row) in enumerate(parts):
        source = pieces[i].at[pl.ds(row, size), pl.ds(places[i], width)]
        ins.append(pltpu.make_async_copy(source, landed.at[pl.ds(j * size, size), :], arrive.at[j]))
        ins[j].start()
    for start in range(0, scales.shape[1], LANES):
        scale_ref[pl.ds(start, LANES)] = scales[:, pl.ds(start, LANES)][0]
    inverse = inverse_ref[...]
    for j, (i, d, row) in enumerate(parts):
        here, there = pl.ds(j * size, size), pl.ds(pl.multiple_of((me ^ d) * rows + row, 16), size)
        ins[j].wait()
        staged[here, :] = ((landed[here, :].astype(jnp.float32) + deltas[here, :]) * inverse).astype(jnp.bfloat16)
        outs.append(pltpu.make_async_copy(staged.at[here, :], out_ref.at[there, pl.ds(offset, width)], leave.at[j]))
        if j:
            outs[j - 1].start()
    outs[-1].start()
    for copy in outs:
        copy.wait()


def cost_of(merged, written, rank, width):
    return pl.CostEstimate(
        flops=2 * merged * rank * width, bytes_accessed=2 * (merged + written) * width, transcendentals=0
    )


def params_of(mebibytes):
    return pltpu.CompilerParams(dimension_semantics=("arbitrary",), vmem_limit_bytes=mebibytes * 1024 * 1024)


def piece_specs(pieces, offset, block):
    return [
        pl.BlockSpec((array.shape[0], block), lambda j, me, at=(offset - start) // block: (0, at + j))
        for _, _, start, array in pieces
    ]


def spans_of(pieces):
    return [(d, row, array.shape[0]) for d, row, _, array in pieces]


def merge_chunk(me, pieces, rows, low_all, high_part, offset, width, previous):
    sources, places = places_of(pieces, rows)
    (all_rows, rank), total = low_all.shape, high_part.shape[1]
    block = LANES if width % LANES == 0 else width
    steps, first = width // block, offset // block
    in_specs = piece_specs(pieces, offset, block)
    in_specs.append(pl.BlockSpec((all_rows, rank), lambda j, me: (0, 0)))
    in_specs.append(pl.BlockSpec((rank, block), lambda j, me: (0, first + j)))
    operands = [*(array for _, _, _, array in pieces), low_all, high_part]
    aliases = {}
    if previous is not None:
        in_specs += [pl.BlockSpec(memory_space=pl.ANY)] * 2
        aliases = {1 + len(operands): 0, 2 + len(operands): 1}
        operands += previous
    return pl.pallas_call(
        functools.partial(merge_kernel, sources, places, spans_of(pieces), rows),
        out_shape=(
            jax.ShapeDtypeStruct((all_rows, total), jnp.bfloat16),
            jax.ShapeDtypeStruct((1, total), jnp.float32),
        ),
        grid_spec=pltpu.PrefetchScalarGridSpec(
            num_scalar_prefetch=1,
            grid=(steps,),
            in_specs=in_specs,
            out_specs=(
                pl.BlockSpec((all_rows, block), lambda j, me: (0, first + j)),
                pl.BlockSpec((1, block), lambda j, me: (0, first + j)),
            ),
            scratch_shapes=[pltpu.VMEM((all_rows, block), jnp.float32)],
        ),
        input_output_aliases=aliases,
        compiler_params=params_of(32),
        cost_estimate=cost_of(all_rows, all_rows, rank, width),
        name=f"merge_{offset}",
    )(me, *operands)


WHOLE = pl.BlockSpec(memory_space=pltpu.VMEM)


def merge_begin(me, pieces, late, peaks, rows, low_all, high_part, offset, width):
    sources, places = places_of(pieces, rows)
    (all_rows, rank), total = low_all.shape, high_part.shape[1]
    early_rows, late_rows = len(sources) * rows, len(late) * rows
    return pl.pallas_call(
        functools.partial(begin_kernel, sources, places, spans_of(pieces), late, rows, offset),
        out_shape=(
            jax.ShapeDtypeStruct((all_rows, total), jnp.bfloat16),
            jax.ShapeDtypeStruct((1, total), jnp.float32),
            jax.ShapeDtypeStruct((1, width), jnp.float32),
            jax.ShapeDtypeStruct((late_rows, width), jnp.float32),
        ),
        grid_spec=pltpu.PrefetchScalarGridSpec(
            num_scalar_prefetch=1,
            grid=(1,),
            in_specs=[
                *piece_specs(pieces, offset, width),
                *[WHOLE] * len(late),
                pl.BlockSpec((all_rows, rank), lambda j, me: (0, 0)),
                pl.BlockSpec((rank, width), lambda j, me: (0, offset // width)),
            ],
            out_specs=(
                pl.BlockSpec(memory_space=pl.ANY),
                pl.BlockSpec((1, width), lambda j, me: (0, offset // width)),
                WHOLE,
                WHOLE,
            ),
            scratch_shapes=[
                pltpu.VMEM((early_rows, width), jnp.float32),
                pltpu.VMEM((early_rows, width), jnp.bfloat16),
                pltpu.SemaphoreType.DMA((len(sources),)),
            ],
        ),
        compiler_params=params_of(32),
        cost_estimate=cost_of(all_rows, all_rows, rank, width),
        name="merge_begin",
    )(me, *(array for _, _, _, array in pieces), *peaks, low_all, high_part)


def merge_finish(me, pieces, rows, deltas, inverse, offset, width, previous):
    late, (all_rows, total) = [d for d, _, _, _ in pieces], previous[0].shape
    places = [offset - start for _, _, start, _ in pieces]
    parts = len(late) * (4 if rows % 64 == 0 else 1)
    return pl.pallas_call(
        functools.partial(finish_kernel, late, places, rows, offset),
        out_shape=(
            jax.ShapeDtypeStruct((all_rows, total), jnp.bfloat16),
            jax.ShapeDtypeStruct((total,), jnp.float32),
        ),
        grid_spec=pltpu.PrefetchScalarGridSpec(
            num_scalar_prefetch=1,
            grid=(1,),
            in_specs=[
                *[pl.BlockSpec(memory_space=pl.ANY)] * len(late),
                *[WHOLE] * 3,
                pl.BlockSpec(memory_space=pl.ANY),
            ],
            out_specs=(pl.BlockSpec(memory_space=pl.ANY), WHOLE),
            scratch_shapes=[
                pltpu.VMEM((len(late) * rows, width), jnp.bfloat16),
                pltpu.VMEM((len(late) * rows, width), jnp.bfloat16),
                pltpu.SemaphoreType.DMA((parts,)),
                pltpu.SemaphoreType.DMA((parts,)),
            ],
        ),
        input_output_aliases={len(late) + 4: 0},
        compiler_params=params_of(16),
        cost_estimate=cost_of(len(late) * rows, len(late) * rows, 1, width),
        name="merge_finish",
    )(me, *(array for _, _, _, array in pieces), deltas, inverse, previous[1], previous[0])


def lead_kernel(d, me_ref, weight_ref, out_ref, sems):
    rows, columns = out_ref.shape
    start = pl.multiple_of((me_ref[0] ^ d) * columns, LANES)
    copies = []
    for i in range(rows // 16):
        here = pl.ds(i * 16, 16)
        source = weight_ref.at[here, pl.ds(start, columns)]
        copies.append(pltpu.make_async_copy(source, out_ref.at[here, :], sems.at[i]))
        copies[i].start()
    for copy in copies:
        copy.wait()


def take_lead(me, weight, d, rows, columns):
    return pl.pallas_call(
        functools.partial(lead_kernel, d),
        out_shape=jax.ShapeDtypeStruct((rows, columns), weight.dtype),
        in_specs=[pl.BlockSpec(memory_space=pltpu.SMEM), pl.BlockSpec(memory_space=pltpu.MemorySpace.HBM)],
        out_specs=WHOLE,
        scratch_shapes=[pltpu.SemaphoreType.DMA((rows // 16,))],
        compiler_params=pltpu.CompilerParams(vmem_limit_bytes=48 * 1024 * 1024),
        name="lead",
    )(me.reshape(1).astype(jnp.int32), weight)


def cut(columns, parts):
    left = columns // LANES - sum(p or 0 for p in parts)
    if columns % LANES or left < 1:
        return [(0, columns)]
    widths = [LANES * (left if p is None else p) for p in parts]
    return [(sum(widths[:i]), width) for i, width in enumerate(widths)]


def shards(n, m, weight_up, low_up, high_up, norm_train, norm_step):
    me, mine = lax.axis_index("zero"), lax.axis_index("width")
    rows, rank = low_up.shape
    columns = weight_up.shape[1] // n
    part, half = rows // m, n // 2

    straight = [d for d in range(n - 1, half - 1, -1) if d % 2 == 0]
    corner = [d for d in range(half, n) if d % 2 == 1]
    near = list(range(1, half))
    final = cut(columns, FINAL)
    offset, width = final[-1]
    ahead = len(final) > 1 and width == LANES
    lead = max(16, rows // 128 * 16)

    def take(weight, d, row, count, start, width):
        here = (row, (me ^ d) * columns + start)
        return d, row, start, lax.dynamic_slice(weight, here, (count, width), allow_negative_indices=False)

    groups = [[(d, 0, rows, 0, columns)] for d in straight]
    if groups:
        groups = [[(straight[0], 0, lead, 0, columns)], [(straight[0], lead, rows - lead, 0, columns)]] + groups[1:]
    groups += [[(d, 0, rows, 0, columns)] for d in near]
    weight, sent, low_own, gain_own, peaks = weight_up, [], low_up, norm_train, []
    for group in groups + [[(d, 0, rows, *span)] for span in final for d in corner]:
        if ahead and not peaks and group[0][0] in corner:
            tops, low_late = [], after(low_up, *arrays)
            for d in corner:
                late = take(weight_up, d, 0, rows, offset, width)[3].astype(jnp.float32)
                high = slice_at(high_up, 1, (me ^ d) * columns + offset, width)
                late += mix_rate * jnp.dot(low_late, high, preferred_element_type=jnp.float32)
                tops.append(jnp.max(jnp.abs(late), axis=0, keepdims=True))
            peaks = [exchange(top, "zero", n, d) for d, top in zip(corner, tops)]
            weight = after(weight, *tops)
        if weight is weight_up and columns % LANES == 0:
            last = [(d, row, start, take_lead(me, weight, d, count, width)) for d, row, count, start, width in group]
        else:
            last = [take(weight, *piece) for piece in group]
        arrays = [array for _, _, _, array in last]
        sent += [(d, row, start, exchange(array, "zero", n, d)) for d, row, start, array in last]
        if weight is weight_up:
            low_own, gain_own = lax.optimization_barrier((low_own, gain_own, *arrays))[:2]
        weight = after(weight, *arrays)
    sent.append(take(weight, 0, 0, rows, 0, columns))

    own = slice_at(low_own, 0, mine * part, part)
    gain = (gain_own + norm_step).astype(jnp.bfloat16)
    own = jnp.concatenate([own.T, gain[None, :]], axis=0)
    pair = jnp.stack([own, exchange(own, "zero", n, half)])
    pairs = jnp.stack([pair] + [exchange(pair, "zero", n, d) for d in range(1, half)], axis=1)
    along = pairs.reshape(n, rank + 1, part)
    spread = jnp.stack([along] + [exchange(along, "width", m, e) for e in range(1, m)])
    spread = jnp.concatenate([slice_at(spread, 0, mine ^ v, 1) for v in range(m)])
    low_all = spread[:, :, :rank, :].transpose(1, 0, 3, 2).reshape(n * rows, rank)
    gains = spread[:, :, rank, :]
    gains = jnp.concatenate([slice_at(gains, 1, me ^ s, 1) for s in range(n)], axis=1)
    serve_norm = gains.transpose(1, 0, 2).reshape(-1)

    high_part = slice_at(high_up, 1, me * columns, columns)
    place = me.reshape(1).astype(jnp.int32)

    def arrived(offset, width, ds):
        fits = lambda start, array: start <= offset and offset + width <= start + array.shape[1]
        return [piece for piece in sent if piece[0] in ds and fits(*piece[2:])]

    result = None
    if ahead:
        early = [d for d in range(n) if d not in corner]
        *result, inverse, deltas = merge_begin(
            place, arrived(offset, width, early), corner, peaks, rows, low_all, high_part, offset, width
        )
    for start, count in final[:-1] if ahead else final:
        pieces = arrived(start, count, range(n))
        result = merge_chunk(place, pieces, rows, low_all, high_part, start, count, result)
    if ahead:
        late = arrived(offset, width, corner)
        ready_up, scale_up = merge_finish(place, late, rows, deltas, inverse, offset, width, result)
    else:
        ready_up, scale_up = result
    return ready_up, scale_up.reshape(-1), serve_norm


def solution(mesh):
    return jax.shard_map(
        functools.partial(shards, mesh.shape["zero"], mesh.shape["width"]),
        mesh=mesh,
        in_specs=(
            P("zero", "width"),
            P("zero", None),
            P(None, "width"),
            P(("zero", "width")),
            P(("zero", "width")),
        ),
        out_specs=(P(None, ("width", "zero")), P(("width", "zero")), P()),
        check_vma=False,
    )
```
